256 devices in a mesh: groups: 2 (over z), seq: 16 (over y, core), head: 8 (over x).
Axes of the slice: x: 8, y: 8, z: 2, core: 2. Of those that a mesh axis runs over, the one named last changes fastest.
The devices are a block of a 8x8x16 slice.
Arguments:
- queries: bfloat16 [4096, 8192], P(('groups', 'seq'), 'head'), parts along dimension 0
- new_keys: bfloat16 [4096, 1024], P(('groups', 'seq'), 'head'), parts along dimension 0, may hold values from -6 to 6
- new_values: bfloat16 [4096, 1024], P(('groups', 'seq'), 'head'), parts along dimension 0, may hold values from -6 to 6
- cache_keys: bfloat16 [32768, 1024], P(('groups', 'seq'), 'head'), parts along dimension 0
- cache_values: bfloat16 [32768, 1024], P(('groups', 'seq'), 'head'), parts along dimension 0, may hold values from -6 to 6
- valid_len: int32 [32], P('groups'), parts along dimension 0, may hold values from 1 to 1024, as said below
- block_of: int32 [32], P('groups'), parts along dimension 0, may hold values from 0 to 15, each once
Outputs:
- attended: bfloat16 [4096, 8192], P(('groups', 'seq'), 'head'), parts along dimension 0
The draws below stay inside these ranges and needn't reach their ends.
There are 2 independent parts, one for each index of `groups`. The reference program is written for one: setup_inputs(seed, part) draws one part's arguments, and reference() takes and returns one part's arrays. A program takes and returns all parts, laid end to end along the dimension named above; each array names one. Nothing has to cross between parts.
Inputs may be any that keep to these rules, and one draw needn't show every extreme that they name: `valid_len`: some shard is full (1024 filled slots) in every draw; slot 0 of every shard is filled. `block_of`: A permutation of the 16 span blocks.
All inputs are finite; a program needn't handle non-finite values.
Results may differ from the reference program's by a relative error of at most 0.0027.
Values may be sent and summed in bfloat16 or wider, within the bound.
A program may use at most 192 MiB of HBM per device.

```python
import math
import jax
import jax.numpy as jnp
from jax import lax

HQ = 64
KV = 8
DH = 128
GROUP = 8
CB = 128
LEN_DEV = 1024
SPAN = 2048
CONTEXT = 16384
N_SEQ = 16


def draw_queries(key, part):
    shape = (SPAN, HQ * DH)
    drawn = jnp.clip(jax.random.normal(key, shape, jnp.float32), -6.0, 6.0)
    return drawn.astype(jnp.bfloat16)


def draw_cache_keys(key, part):
    shape = (CONTEXT, KV * DH)
    drawn = jnp.clip(jax.random.normal(key, shape, jnp.float32), -6.0, 6.0)
    return drawn.astype(jnp.bfloat16)


def draw_valid_len(key, part):
    filled = jax.random.randint(jax.random.fold_in(key, 3), (N_SEQ,), 1, LEN_DEV + 1)
    full_one = jax.random.randint(jax.random.fold_in(key, 5), (), 0, N_SEQ)
    return filled.at[full_one].set(LEN_DEV).astype(jnp.int32)


def shard_levels(rng, shape, cuts, smallest, largest):
    factor_of, own = 1.0, jax.random.fold_in(rng, 6)
    for axis_at, parts in cuts:
        heights = jnp.exp(jax.random.uniform(jax.random.fold_in(own, axis_at), (parts,), jnp.float32, smallest / len(cuts), largest / len(cuts)))
        factor_of = factor_of * jnp.repeat(heights, shape[axis_at] // parts).reshape([-1 if axis == axis_at else 1 for axis in range(len(shape))])
    return factor_of


def bell_draw(key, dims, scale, limit, pieces=(), kind=jnp.bfloat16):
    values = scale * jax.random.normal(key, dims, jnp.float32)
    if pieces:
        values = values * shard_levels(key, dims, pieces, -0.22, 0.18)
    return jnp.clip(values, -limit, limit).astype(kind)


def setup_inputs(seed: int = 0, part: int = 0) -> dict:
    streams_of = jax.random.split(jax.random.key(seed), 8)
    part_splits = jax.random.split(jax.random.fold_in(streams_of[7], part), 8)
    queries = draw_queries(jax.random.fold_in(jax.random.fold_in(streams_of[7], part), 71), part)
    new_keys = bell_draw(part_splits[1], (SPAN, KV * DH), 1.0, 6.0, ((0, 16), (1, 8)))
    new_values = bell_draw(part_splits[2], (SPAN, KV * DH), 1.0, 6.0, ((0, 16), (1, 8)))
    cache_keys = draw_cache_keys(jax.random.fold_in(jax.random.fold_in(streams_of[7], part), 71), part)
    cache_values = bell_draw(part_splits[4], (CONTEXT, KV * DH), 1.0, 6.0, ((0, 16), (1, 8)))
    valid_len = draw_valid_len(jax.random.fold_in(jax.random.fold_in(streams_of[7], part), 71), part)
    block_of = jax.random.permutation(part_splits[6], N_SEQ).astype(jnp.int32)
    return dict(queries=queries, new_keys=new_keys, new_values=new_values, cache_keys=cache_keys, cache_values=cache_values, valid_len=valid_len, block_of=block_of)


def reference(queries, new_keys, new_values, cache_keys, cache_values, valid_len, block_of):
    span = CB * N_SEQ
    context = LEN_DEV * N_SEQ
    rows = jnp.arange(span, dtype=jnp.int32)
    query_pos = block_of[rows // CB].astype(jnp.int32) * CB + rows % CB
    places = jnp.arange(context, dtype=jnp.int32)
    cache_live = (places % LEN_DEV) < valid_len[places // LEN_DEV]
    key_pos = jnp.concatenate([jnp.full((context,), -1, jnp.int32), query_pos])
    key_live = jnp.concatenate([cache_live, jnp.ones((span,), bool)])
    keys_all = jnp.concatenate([cache_keys, new_keys], 0).astype(jnp.float32).reshape(-1, KV, DH)
    values_cache = cache_values.astype(jnp.float32).reshape(N_SEQ, LEN_DEV, KV, DH)
    values_span = new_values.astype(jnp.float32).reshape(N_SEQ, CB, KV, DH)
    width = math.gcd(span, 16)
    count = span // width
    query_blocks = queries.astype(jnp.float32).reshape(count, width, KV, GROUP, DH)
    pos_blocks = query_pos.reshape(count, width)

    def one_block(item):
        block, pos = item
        scores = jnp.einsum("rkgd,nkd->rkgn", block, keys_all) * (DH ** -0.5)
        seen = (key_live[None, :] & (key_pos[None, :] <= pos[:, None]))[:, None, None, :]
        masked = jnp.where(seen, scores, -1.0e30)
        lead = masked.shape[:3]
        cache_part = masked[..., :context].reshape(lead + (N_SEQ, LEN_DEV))
        span_part = masked[..., context:].reshape(lead + (N_SEQ, CB))
        local = jnp.maximum(jnp.max(cache_part, axis=-1), jnp.max(span_part, axis=-1))
        local_full = jnp.concatenate([jnp.repeat(local, LEN_DEV, axis=-1), jnp.repeat(local, CB, axis=-1)], -1)
        weights = jnp.where(seen, jnp.exp(scores - local_full), 0.0)
        rounded = lax.optimization_barrier(weights.astype(jnp.bfloat16)).astype(jnp.float32)
        weights_cache = weights[..., :context].reshape(lead + (N_SEQ, LEN_DEV))
        weights_span = weights[..., context:].reshape(lead + (N_SEQ, CB))
        part_total = jnp.sum(weights_cache, axis=-1) + jnp.sum(weights_span, axis=-1)
        rounded_cache = rounded[..., :context].reshape(lead + (N_SEQ, LEN_DEV))
        rounded_span = rounded[..., context:].reshape(lead + (N_SEQ, CB))
        part_numer = jnp.einsum("rkgsl,slkd->rkgsd", rounded_cache, values_cache)
        part_numer = part_numer + jnp.einsum("rkgsc,sckd->rkgsd", rounded_span, values_span)
        top = jnp.max(local, axis=-1)
        factor = jnp.exp(local - top[..., None])
        numer = jnp.sum(part_numer * factor[..., None], axis=-2)
        total = jnp.sum(part_total * factor, axis=-1)
        return (numer / total[..., None]).astype(jnp.bfloat16).reshape(width, -1)

    result = lax.map(one_block, (query_blocks, pos_blocks))
    return result.reshape(span, HQ * DH)
```

```python
import functools
import math

import jax
import jax.numpy as jnp
from jax import lax
from jax.experimental import pallas as pl
from jax.experimental.pallas import tpu as pltpu
from jax.sharding import PartitionSpec as P

DH = 128
GROUP = 8
NEGATIVE = -1e30
FACTOR = DH ** (-0.5) * math.log2(math.e)
WIDE = 256


def kernel(
    n,
    q_hbm, nk_hbm, nv_hbm, ck_hbm, cv_hbm, vl_ref, bo_ref,
    out_ref,
    kv, qs, s_ref, p_ref, acc, best, total,
    q_sem, own_sem, ring_send, ring_recv, pair_send, pair_recv,
):
    chips = n // 2
    far = chips // 2
    length = ck_hbm.shape[0]
    span = nk_hbm.shape[0]
    rows = length + span
    half = rows // 2
    me = lax.axis_index("seq")
    chip, core = me // 2, me % 2
    right = lax.rem(chip + 1, chips) * 2 + core
    left = lax.rem(chip + chips - 1, chips) * 2 + core
    pair = chip * 2 + 1 - core
    last = 2 * far - 1

    barrier = pltpu.get_barrier_semaphore()
    for peer in (right, left, pair):
        pl.semaphore_signal(
            barrier, inc=1, device_id={"seq": peer},
            device_id_type=pl.DeviceIdType.MESH,
        )

    def own_copies(part):
        cache, fresh = ((ck_hbm, nk_hbm), (cv_hbm, nv_hbm))[part]
        return (
            pltpu.make_async_copy(
                cache, kv.at[part, 0, 0, pl.ds(0, length)], own_sem.at[part, 0]
            ),
            pltpu.make_async_copy(
                fresh, kv.at[part, 0, 0, pl.ds(length, span)], own_sem.at[part, 1]
            ),
        )

    q_copies = [
        pltpu.make_async_copy(
            q_hbm.at[:, pl.ds(h * DH, DH)], qs.at[pl.ds(h * span, span)], q_sem.at[h]
        )
        for h in range(GROUP)
    ]
    for part in range(2):
        for c in own_copies(part):
            c.start()
    for c in q_copies:
        c.start()

    def ring(step, part, way):
        at = 0 if step == 1 else 2 * (step - 1) - 1 + way
        to = 2 * step - 1 + way if step < far else last
        first, count = (0, rows) if step < far else (way * half, half)
        return pltpu.make_async_remote_copy(
            src_ref=kv.at[part, 0, at, pl.ds(first, count)],
            dst_ref=kv.at[part, 0, to, pl.ds(first, count)],
            send_sem=ring_send.at[step - 1, part, way],
            recv_sem=ring_recv.at[step - 1, part, way],
            device_id={"seq": (right, left)[way]},
            device_id_type=pl.DeviceIdType.MESH,
        )

    def to_pair(at, part, way=0):
        first, count = (0, rows) if at < last else (way * half, half)
        return pltpu.make_async_remote_copy(
            src_ref=kv.at[part, 0, at, pl.ds(first, count)],
            dst_ref=kv.at[part, 1, at, pl.ds(first, count)],
            send_sem=pair_send.at[at + way, part],
            recv_sem=pair_recv.at[at + way, part],
            device_id={"seq": pair},
            device_id_type=pl.DeviceIdType.MESH,
        )

    acc[...] = jnp.zeros_like(acc)
    best[...] = jnp.full_like(best, NEGATIVE)
    total[...] = jnp.zeros_like(total)

    my_block = bo_ref[me]

    def process(side, at):
        dist = (at + 1) // 2
        offset = jnp.where(at % 2 == 1, chips - dist, dist)
        shard = lax.rem(chip + offset, chips) * 2 + lax.rem(core + side, 2)
        filled = vl_ref[shard]
        block = bo_ref[shard]
        slope = jnp.where(block == my_block, 1, 0)
        level = jnp.where(block < my_block, span - 1, jnp.where(block == my_block, 0, -1))
        at_row = lax.broadcasted_iota(jnp.int32, (rows, WIDE), 0)
        at_col = lax.broadcasted_iota(jnp.int32, (span, WIDE), 1) % span

        def columns(b, _):
            cols = pl.ds(pl.multiple_of(b * WIDE, WIDE), WIDE)
            s = lax.dot_general(
                kv[0, side, at], qs[cols, :], (((1,), (1,)), ((), ())),
                preferred_element_type=jnp.float32,
            )
            cache_seen = at_row[:length] < filled
            span_seen = at_row[:span] <= at_col * slope + level
            s_cache = jnp.where(cache_seen, s[:length], NEGATIVE)
            s_span = jnp.where(span_seen, s[length:], NEGATIVE)
            s_ref[:length, :] = s_cache
            s_ref[length:, :] = s_span
            local = jnp.maximum(
                jnp.max(s_cache, axis=0, keepdims=True),
                jnp.max(s_span, axis=0, keepdims=True),
            )
            w = jnp.exp2((s_ref[...] - local) * FACTOR)
            part_total = jnp.sum(w, axis=0, keepdims=True)
            p_ref[...] = w.astype(jnp.bfloat16)
            numer = lax.dot_general(
                kv[1, side, at], p_ref[...], (((0,), (0,)), ((), ())),
                preferred_element_type=jnp.float32,
            )
            old = best[:, cols]
            newest = jnp.maximum(old, local)
            keep = jnp.exp2((old - newest) * FACTOR)
            fresh = jnp.exp2((local - newest) * FACTOR)
            best[:, cols] = newest
            total[:, cols] = total[:, cols] * keep + part_total * fresh
            acc[:, cols] = acc[:, cols] * keep + numer * fresh
            return 0

        lax.fori_loop(0, GROUP * span // WIDE, columns, 0)

    def process_two(side, at):
        lax.fori_loop(0, 2, lambda i, _: (process(side, at + i), 0)[1], 0)

    pl.semaphore_wait(barrier, 3)
    for part in range(2):
        for c in own_copies(part):
            c.wait()
        for way in range(2):
            ring(1, part, way).start()
        to_pair(0, part).start()
    for c in q_copies:
        c.wait()
    process(0, 0)
    for part in range(2):
        to_pair(0, part).wait_recv()
    process(1, 0)
    for step in range(1, far):
        for part in range(2):
            for way in range(2):
                ring(step, part, way).wait_recv()
                if step + 1 < far or True:
                    if step + 1 <= far:
                        ring(step + 1, part, way).start()
                to_pair(2 * step - 1 + way, part).start()
        process_two(0, 2 * step - 1)
        for part in range(2):
            for way in range(2):
                to_pair(2 * step - 1 + way, part).wait_recv()
        process_two(1, 2 * step - 1)
    for part in range(2):
        for way in range(2):
            ring(far, part, way).wait_recv()
            to_pair(last, part, way).start()
    process(0, last)
    for part in range(2):
        for way in range(2):
            to_pair(last, part, way).wait_recv()
    process(1, last)

    for h in range(GROUP):
        cols = pl.ds(h * span, span)
        out_ref[:, pl.ds(h * DH, DH)] = (
            (acc[:, cols] / total[:, cols]).T.astype(out_ref.dtype)
        )

    for part in range(2):
        for step in range(1, far + 1):
            for way in range(2):
                ring(step, part, way).wait_send()
        for at in range(last):
            to_pair(at, part).wait_send()
        for way in range(2):
            to_pair(last, part, way).wait_send()


def solution(mesh):
    n = mesh.shape["seq"]

    def on_device(queries, new_keys, new_values, cache_keys, cache_values, valid_len, block_of):
        span = queries.shape[0]
        rows = cache_keys.shape[0] + span
        slots = n // 2
        any_spec = pl.BlockSpec(memory_space=pl.ANY)
        smem = pl.BlockSpec(memory_space=pltpu.SMEM)
        return pl.pallas_call(
            functools.partial(kernel, n),
            out_shape=jax.ShapeDtypeStruct(queries.shape, jnp.bfloat16),
            in_specs=[any_spec] * 5 + [smem] * 2,
            out_specs=pl.BlockSpec(memory_space=pltpu.VMEM),
            scratch_shapes=[
                pltpu.VMEM((2, 2, slots, rows, DH), jnp.bfloat16),
                pltpu.VMEM((GROUP * span, DH), jnp.bfloat16),
                pltpu.VMEM((rows, WIDE), jnp.float32),
                pltpu.VMEM((rows, WIDE), jnp.bfloat16),
                pltpu.VMEM((DH, GROUP * span), jnp.float32),
                pltpu.VMEM((1, GROUP * span), jnp.float32),
                pltpu.VMEM((1, GROUP * span), jnp.float32),
                pltpu.SemaphoreType.DMA((GROUP,)),
                pltpu.SemaphoreType.DMA((2, 2)),
                pltpu.SemaphoreType.DMA((slots // 2, 2, 2)),
                pltpu.SemaphoreType.DMA((slots // 2, 2, 2)),
                pltpu.SemaphoreType.DMA((slots + 1, 2)),
                pltpu.SemaphoreType.DMA((slots + 1, 2)),
            ],
            compiler_params=pltpu.CompilerParams(
                collective_id=0, has_side_effects=True,
                vmem_limit_bytes=60 * 1024 * 1024,
            ),
        )(queries, new_keys, new_values, cache_keys, cache_values, valid_len, block_of)

    rows_spec = P(("groups", "seq"), "head")
    return jax.shard_map(
        on_device,
        mesh=mesh,
        in_specs=(rows_spec,) * 5 + (P("groups"), P("groups")),
        out_specs=rows_spec,
        check_vma=False,
    )
```

```python
import functools
import math

import jax
import jax.numpy as jnp
from jax import lax
from jax.experimental import pallas as pl
from jax.experimental.pallas import tpu as pltpu
from jax.sharding import PartitionSpec as P

DH = 128
GROUP = 8
NEGATIVE = -1e30
FACTOR = DH ** (-0.5) * math.log2(math.e)
WIDE = 256
TALL = 384


def kernel(
    n,
    q_hbm, nk_hbm, nv_hbm, ck_hbm, cv_hbm, vl_ref, bo_ref,
    out_ref,
    kv, qs, vt, bias, s_ref, weights, tops, parts, acc, best, total,
    hello, q_sem, own_sem, ring_send, ring_recv, pair_send, pair_recv,
):
    chips = n // 2
    far = chips // 2
    length = ck_hbm.shape[0]
    span = nk_hbm.shape[0]
    rows = length + span
    half = rows // 2
    me = lax.axis_index("seq")
    chip, core = me // 2, me % 2
    right = lax.rem(chip + 1, chips) * 2 + core
    left = lax.rem(chip + chips - 1, chips) * 2 + core
    pair = chip * 2 + 1 - core
    last = 2 * far - 1

    barrier = pltpu.get_barrier_semaphore()

    def greet(peer):
        pl.semaphore_signal(
            barrier, inc=1, device_id={"seq": peer}, device_id_type=pl.DeviceIdType.MESH
        )

    greet(right)
    greet(left)
    pl.when(core == 1)(lambda: greet(pair))

    def own_copies(part):
        cache, fresh = ((ck_hbm, nk_hbm), (cv_hbm, nv_hbm))[part]
        return (
            pltpu.make_async_copy(
                cache, kv.at[part, 0, 0, pl.ds(0, length)], own_sem.at[part, 0]
            ),
            pltpu.make_async_copy(
                fresh, kv.at[part, 0, 0, pl.ds(length, span)], own_sem.at[part, 1]
            ),
        )

    q_copies = [
        pltpu.make_async_copy(
            q_hbm.at[:, pl.ds(h * DH, DH)],
            qs.at[pl.ds(h * span, span), pl.ds(0, DH)],
            q_sem.at[h],
        )
        for h in range(GROUP)
    ]
    for part in range(2):
        for c in own_copies(part):
            c.start()
    for c in q_copies:
        c.start()

    def ring(step, part, way):
        at = 0 if step == 1 else 2 * (step - 1) - 1 + way
        to = 2 * step - 1 + way if step < far else last
        first, count = (0, rows) if step < far else (way * half, half)
        return pltpu.make_async_remote_copy(
            src_ref=kv.at[part, 0, at, pl.ds(first, count)],
            dst_ref=kv.at[part, 0, to, pl.ds(first, count)],
            send_sem=ring_send.at[step - 1, part, way],
            recv_sem=ring_recv.at[step - 1, part, way],
            device_id={"seq": (right, left)[way]},
            device_id_type=pl.DeviceIdType.MESH,
        )

    def to_pair(at, part, way=0):
        first, count = (way * half, half) if at is last else (0, rows)
        return pltpu.make_async_remote_copy(
            src_ref=kv.at[part, 0, at, pl.ds(first, count)],
            dst_ref=kv.at[part, 1, at, pl.ds(first, count)],
            send_sem=pair_send.at[at + way, part],
            recv_sem=pair_recv.at[at + way, part],
            device_id={"seq": pair},
            device_id_type=pl.DeviceIdType.MESH,
        )

    acc[...] = jnp.zeros_like(acc)
    best[...] = jnp.full_like(best, NEGATIVE)
    total[...] = jnp.zeros_like(total)
    place = lax.broadcasted_iota(jnp.int32, (span, DH), 0)
    lane = lax.broadcasted_iota(jnp.int32, (span, DH), 1)
    marks = jnp.where((lane > place) | (lane == 0), 1.0, 0.0).astype(jnp.bfloat16)
    for h in range(GROUP):
        qs[pl.ds(h * span, span), pl.ds(DH, DH)] = marks

    my_block = bo_ref[me]
    blocks = GROUP * span // WIDE

    def attend(side, at, weigh_into, finish):
        dist = (at + 1) // 2
        offset = jnp.where(at % 2 == 1, chips - dist, dist)
        shard = lax.rem(chip + offset, chips) * 2 + lax.rem(core + side, 2)
        filled = vl_ref[shard]
        block = bo_ref[shard]
        row = lax.broadcasted_iota(jnp.int32, (length, DH), 0)
        col = lax.broadcasted_iota(jnp.int32, (length, DH), 1)
        bias[pl.ds(0, length), :] = jnp.where(
            (col == 0) & (row >= filled), NEGATIVE, 0.0
        ).astype(jnp.bfloat16)
        hidden_col = jnp.where(block == my_block, place, jnp.where(block < my_block, -1, 0))
        hidden = (lane == hidden_col) & ((place > 0) | (block > my_block))
        bias[pl.ds(length, span), :] = jnp.where(hidden, NEGATIVE, 0.0).astype(jnp.bfloat16)

        local, sums = {}, {}

        def score(b, first):
            s = lax.dot_general(
                jnp.concatenate(
                    [kv[0, side, at, pl.ds(first, TALL), :], bias[pl.ds(first, TALL), :]], axis=1
                ),
                qs[pl.ds(b * WIDE, WIDE), :],
                (((1,), (1,)), ((), ())),
                preferred_element_type=jnp.float32,
            )
            s_ref[pl.ds(first, TALL), :] = s
            high = jnp.max(s.reshape(TALL // 8, 8, WIDE), axis=0)
            local[b] = jnp.maximum(local[b], high) if b in local else high

        def weigh(b, first):
            w = jnp.exp2((s_ref[pl.ds(first, span), :] - local[b]) * FACTOR)
            part = jnp.sum(w.reshape(span // 8, 8, WIDE), axis=0)
            sums[b] = sums[b] + part if b in sums else part
            weigh_into(b)[pl.ds(first, span), :] = w.astype(jnp.bfloat16)

        for b in range(blocks + 1):
            for first in range(0, rows, TALL):
                if b > 0:
                    for inner in range(first, first + TALL, span):
                        weigh(b - 1, inner)
                if b < blocks:
                    score(b, first)
            if b < blocks:
                local[b] = jnp.max(local[b], axis=0, keepdims=True)
            if b > 0:
                finish(b - 1, local[b - 1], jnp.sum(sums[b - 1], axis=0, keepdims=True))

    def combine(b, weighted, local, part_total):
        cols = pl.ds(b * WIDE, WIDE)
        numer = jnp.dot(vt[...], weighted, preferred_element_type=jnp.float32)
        old = best[:, cols]
        newest = jnp.maximum(old, local)
        keep = jnp.exp2((old - newest) * FACTOR)
        fresh = jnp.exp2((local - newest) * FACTOR)
        best[:, cols] = newest
        total[:, cols] = total[:, cols] * keep + part_total * fresh
        acc[:, cols] = acc[:, cols] * keep + numer * fresh

    def weigh_shard(side, at):
        def finish(b, local, part_total):
            cols = pl.ds(b * WIDE, WIDE)
            tops[side, at, :, cols] = local
            parts[side, at, :, cols] = part_total

        attend(side, at, lambda b: weights.at[side, at, b], finish)

    def combine_shard(side, at):
        vt[...] = kv[1, side, at].T
        for b in range(blocks):
            cols = pl.ds(b * WIDE, WIDE)
            combine(b, weights[side, at, b], tops[side, at, :, cols], parts[side, at, :, cols])

    def receive(step, part):
        for way in (1, 0):
            ring(step, part, way).wait_recv()
            if step < far:
                ring(step + 1, part, way).start()
        for way in (1, 0):
            if step < far:
                if step > 1:
                    to_pair(2 * step - 1 + way, part).start()
            else:
                to_pair(last, part, way).start()

    def met_pair():
        receive(1, 1)

        @pl.when(core == 1)
        def _():
            pl.semaphore_wait(hello, 1)
            for part in range(2):
                to_pair(0, part).start()

        for at in (2, 1):
            for part in range(2):
                to_pair(at, part).start()

    def last_of_pair(part):
        for way in range(2):
            to_pair(last, part, way).wait_recv()

    turns = []

    def turn(what, side, at, action=None):
        turns.append((what, side, at, action))

    turn(0, 0, 0)
    turn(1, 0, 0)
    turn(0, 0, 2, lambda: receive(1, 0))
    turn(0, 0, 1)
    turn(1, 0, 2, met_pair)
    turn(1, 0, 1)
    turn(0, 1, 0)
    turn(1, 1, 0)
    behind = []
    for step in range(2, far):
        new = [2 * step, 2 * step - 1]
        turn(0, 0, new[0], functools.partial(receive, step, 0))
        turn(0, 0, new[1])
        for at in behind:
            turn(0, 1, at)
        if step + 1 == far and far > 2 and step > 2:
            turn(0, 1, new[0])
            early = [new[0]]
        else:
            early = []
        turn(1, 0, new[0], functools.partial(receive, step, 1))
        turn(1, 0, new[1])
        for at in [2 * step - 2] * (step > 2) + behind + early:
            turn(1, 1, at)
        if step + 1 < far:
            for at in (2 * step - 2, 2 * step - 3):
                turn(0, 1, at)
                turn(1, 1, at)
            turn(0, 1, new[0])
            behind = [new[1]]
        else:
            for at in new:
                if at not in early:
                    turn(0, 1, at)
                    turn(1, 1, at)
    turn(0, 0, last, lambda: receive(far, 0))
    turn(0, 1, last, lambda: last_of_pair(0))
    turn(1, 0, last, lambda: receive(far, 1))
    turn(1, 1, last, lambda: last_of_pair(1))

    def one(i, _):
        what = i * 0
        side = i * 0
        at = i * 0
        for k, (w, a, b, action) in enumerate(turns):
            what = jnp.where(i == k, w, what)
            side = jnp.where(i == k, a, side)
            at = jnp.where(i == k, b, at)
            if action is not None:
                pl.when(i == k)(action)

        for part in range(2):

            @pl.when((what == part) & (side == 1) & (at != last))
            def _():
                to_pair(at, part).wait_recv()

        pl.when(what == 0)(lambda: weigh_shard(side, at))
        pl.when(what == 1)(lambda: combine_shard(side, at))
        return 0

    pl.semaphore_wait(barrier, 3 - core)

    @pl.when(core == 0)
    def _():
        pl.semaphore_signal(
            hello, inc=1, device_id={"seq": pair}, device_id_type=pl.DeviceIdType.MESH
        )

    for part in range(2):
        for c in own_copies(part):
            c.wait()
        for way in range(2):
            ring(1, part, way).start()

    @pl.when(core == 0)
    def _():
        for part in range(2):
            to_pair(0, part).start()

    for c in q_copies:
        c.wait()
    lax.fori_loop(0, len(turns), one, 0)

    for h in range(GROUP):
        cols = pl.ds(h * span, span)
        out_ref[:, pl.ds(h * DH, DH)] = (
            (acc[:, cols] / total[:, cols]).T.astype(out_ref.dtype)
        )

    for part in range(2):
        for step in range(1, far + 1):
            for way in range(2):
                ring(step, part, way).wait_send()
        for at in range(last):
            to_pair(at, part).wait_send()
        for way in range(2):
            to_pair(last, part, way).wait_send()


def solution(mesh):
    n = mesh.shape["seq"]

    def on_device(queries, new_keys, new_values, cache_keys, cache_values, valid_len, block_of):
        span = queries.shape[0]
        rows = cache_keys.shape[0] + span
        slots = n // 2
        any_spec = pl.BlockSpec(memory_space=pl.ANY)
        smem = pl.BlockSpec(memory_space=pltpu.SMEM)
        return pl.pallas_call(
            functools.partial(kernel, n),
            out_shape=jax.ShapeDtypeStruct(queries.shape, jnp.bfloat16),
            in_specs=[any_spec] * 5 + [smem] * 2,
            out_specs=pl.BlockSpec(memory_space=pltpu.VMEM),
            scratch_shapes=[
                pltpu.VMEM((2, 2, slots, rows, DH), jnp.bfloat16),
                pltpu.VMEM((GROUP * span, 2 * DH), jnp.bfloat16),
                pltpu.VMEM((DH, rows), jnp.bfloat16),
                pltpu.VMEM((rows, DH), jnp.bfloat16),
                pltpu.VMEM((rows, WIDE), jnp.float32),
                pltpu.VMEM((2, slots, GROUP * span // WIDE, rows, WIDE), jnp.bfloat16),
                pltpu.VMEM((2, slots, 1, GROUP * span), jnp.float32),
                pltpu.VMEM((2, slots, 1, GROUP * span), jnp.float32),
                pltpu.VMEM((DH, GROUP * span), jnp.float32),
                pltpu.VMEM((1, GROUP * span), jnp.float32),
                pltpu.VMEM((1, GROUP * span), jnp.float32),
                pltpu.SemaphoreType.REGULAR,
                pltpu.SemaphoreType.DMA((GROUP,)),
                pltpu.SemaphoreType.DMA((2, 2)),
                pltpu.SemaphoreType.DMA((slots // 2, 2, 2)),
                pltpu.SemaphoreType.DMA((slots // 2, 2, 2)),
                pltpu.SemaphoreType.DMA((slots + 1, 2)),
                pltpu.SemaphoreType.DMA((slots + 1, 2)),
            ],
            compiler_params=pltpu.CompilerParams(
                collective_id=0, has_side_effects=True,
                vmem_limit_bytes=60 * 1024 * 1024,
            ),
        )(queries, new_keys, new_values, cache_keys, cache_values, valid_len, block_of)

    rows_spec = P(("groups", "seq"), "head")
    return jax.shard_map(
        on_device,
        mesh=mesh,
        in_specs=(rows_spec,) * 5 + (P("groups"), P("groups")),
        out_specs=rows_spec,
        check_vma=False,
    )
```

```python
import functools
import math

import jax
import jax.numpy as jnp
from jax import lax
from jax.experimental import pallas as pl
from jax.experimental.pallas import tpu as pltpu
from jax.sharding import PartitionSpec as P

DH = 128
GROUP = 8
NEGATIVE = -1e30
FACTOR = DH ** (-0.5) * math.log2(math.e)
WIDE = 256
TALL = 384

TURNS = (
    (
        (3, 0,),
        (17, 9,),
        (18, 10, 7, 23,),
        (33, 25, 15,),
        (34, 26, 39, 31,),
        (49, 41, 53, 45,),
        (50, 42, 54, 46,),
        (57,),
        (61,),
        (58,),
        (62,),
    ),
    (
        (3, 7,),
        (17, 9,),
        (18, 10, 23, 0,),
        (33, 25, 15,),
        (34, 26, 39, 31,),
        (49, 41, 53, 45,),
        (50, 42, 54, 46,),
        (57,),
        (61,),
        (58,),
        (62,),
    ),
)


def kernel(
    n,
    q_hbm, nk_hbm, nv_hbm, ck_hbm, cv_hbm, vl_ref, bo_ref,
    out_ref,
    kv, qs, vt, bias, s_ref, p_even, p_odd, weights, tops, parts, acc, best, total,
    hello, q_sem, own_sem, ring_send, ring_recv, pair_send, pair_recv,
):
    chips = n // 2
    far = chips // 2
    length = ck_hbm.shape[0]
    span = nk_hbm.shape[0]
    rows = length + span
    half = rows // 2
    me = lax.axis_index("seq")
    chip, core = me // 2, me % 2
    right = lax.rem(chip + 1, chips) * 2 + core
    left = lax.rem(chip + chips - 1, chips) * 2 + core
    pair = chip * 2 + 1 - core
    last = 2 * far - 1

    barrier = pltpu.get_barrier_semaphore()

    def greet(peer):
        pl.semaphore_signal(
            barrier, inc=1, device_id={"seq": peer}, device_id_type=pl.DeviceIdType.MESH
        )

    greet(right)
    greet(left)
    pl.when(core == 1)(lambda: greet(pair))

    def own_copies(part):
        cache, fresh = ((ck_hbm, nk_hbm), (cv_hbm, nv_hbm))[part]
        return (
            pltpu.make_async_copy(
                cache, kv.at[part, 0, 0, pl.ds(0, length)], own_sem.at[part, 0]
            ),
            pltpu.make_async_copy(
                fresh, kv.at[part, 0, 0, pl.ds(length, span)], own_sem.at[part, 1]
            ),
        )

    q_copies = [
        pltpu.make_async_copy(
            q_hbm.at[:, pl.ds(h * DH, DH)],
            qs.at[pl.ds(h * span, span), pl.ds(0, DH)],
            q_sem.at[h],
        )
        for h in range(GROUP)
    ]
    for part in range(2):
        for c in own_copies(part):
            c.start()
    for c in q_copies:
        c.start()

    def ring(step, part, way):
        at = 0 if step == 1 else 2 * (step - 1) - 1 + way
        to = 2 * step - 1 + way if step < far else last
        first, count = (0, rows) if step < far else (way * half, half)
        return pltpu.make_async_remote_copy(
            src_ref=kv.at[part, 0, at, pl.ds(first, count)],
            dst_ref=kv.at[part, 0, to, pl.ds(first, count)],
            send_sem=ring_send.at[step - 1, part, way],
            recv_sem=ring_recv.at[step - 1, part, way],
            device_id={"seq": (right, left)[way]},
            device_id_type=pl.DeviceIdType.MESH,
        )

    def to_pair(at, part, way=0):
        first, count = (way * half, half) if at is last else (0, rows)
        return pltpu.make_async_remote_copy(
            src_ref=kv.at[part, 0, at, pl.ds(first, count)],
            dst_ref=kv.at[part, 1, at, pl.ds(first, count)],
            send_sem=pair_send.at[at + way, part],
            recv_sem=pair_recv.at[at + way, part],
            device_id={"seq": pair},
            device_id_type=pl.DeviceIdType.MESH,
        )

    acc[...] = jnp.zeros_like(acc)
    best[...] = jnp.full_like(best, NEGATIVE)
    total[...] = jnp.zeros_like(total)
    place = lax.broadcasted_iota(jnp.int32, (span, DH), 0)
    lane = lax.broadcasted_iota(jnp.int32, (span, DH), 1)
    marks = jnp.where((lane > place) | (lane == 0), 1.0, 0.0).astype(jnp.bfloat16)
    for h in range(GROUP):
        qs[pl.ds(h * span, span), pl.ds(DH, DH)] = marks

    my_block = bo_ref[me]
    blocks = GROUP * span // WIDE
    p_refs = (p_even, p_odd)

    def attend(side, at, weigh_into, finish):
        dist = (at + 1) // 2
        offset = jnp.where(at % 2 == 1, chips - dist, dist)
        shard = lax.rem(chip + offset, chips) * 2 + lax.rem(core + side, 2)
        filled = vl_ref[shard]
        block = bo_ref[shard]
        row = lax.broadcasted_iota(jnp.int32, (length, DH), 0)
        col = lax.broadcasted_iota(jnp.int32, (length, DH), 1)
        bias[pl.ds(0, length), :] = jnp.where(
            (col == 0) & (row >= filled), NEGATIVE, 0.0
        ).astype(jnp.bfloat16)
        hidden_col = jnp.where(block == my_block, place, jnp.where(block < my_block, -1, 0))
        hidden = (lane == hidden_col) & ((place > 0) | (block > my_block))
        bias[pl.ds(length, span), :] = jnp.where(hidden, NEGATIVE, 0.0).astype(jnp.bfloat16)

        local, sums = {}, {}

        def score(b, first):
            s = lax.dot_general(
                jnp.concatenate(
                    [kv[0, side, at, pl.ds(first, TALL), :], bias[pl.ds(first, TALL), :]], axis=1
                ),
                qs[pl.ds(b * WIDE, WIDE), :],
                (((1,), (1,)), ((), ())),
                preferred_element_type=jnp.float32,
            )
            s_ref[pl.ds(first, TALL), :] = s
            high = jnp.max(s.reshape(TALL // 8, 8, WIDE), axis=0)
            local[b] = jnp.maximum(local[b], high) if b in local else high

        def weigh(b, first):
            w = jnp.exp2((s_ref[pl.ds(first, span), :] - local[b]) * FACTOR)
            part = jnp.sum(w.reshape(span // 8, 8, WIDE), axis=0)
            sums[b] = sums[b] + part if b in sums else part
            weigh_into(b)[pl.ds(first, span), :] = w.astype(jnp.bfloat16)

        for b in range(blocks + 1):
            for first in range(0, rows, TALL):
                if b > 0:
                    for inner in range(first, first + TALL, span):
                        weigh(b - 1, inner)
                if b < blocks:
                    score(b, first)
            if b < blocks:
                local[b] = jnp.max(local[b], axis=0, keepdims=True)
            if b > 0:
                finish(b - 1, local[b - 1], jnp.sum(sums[b - 1], axis=0, keepdims=True))

    def combine(b, weighted, local, part_total):
        cols = pl.ds(b * WIDE, WIDE)
        numer = jnp.dot(vt[...], weighted, preferred_element_type=jnp.float32)
        old = best[:, cols]
        newest = jnp.maximum(old, local)
        keep = jnp.exp2((old - newest) * FACTOR)
        fresh = jnp.exp2((local - newest) * FACTOR)
        best[:, cols] = newest
        total[:, cols] = total[:, cols] * keep + part_total * fresh
        acc[:, cols] = acc[:, cols] * keep + numer * fresh

    def weigh_shard(side, at):
        def finish(b, local, part_total):
            cols = pl.ds(b * WIDE, WIDE)
            tops[side, at, :, cols] = local
            parts[side, at, :, cols] = part_total

        attend(side, at, lambda b: weights.at[side, at, b], finish)

    def combine_shard(side, at):
        vt[...] = kv[1, side, at].T
        for b in range(blocks):
            cols = pl.ds(b * WIDE, WIDE)
            combine(b, weights[side, at, b], tops[side, at, :, cols], parts[side, at, :, cols])

    def whole_shard(side, at):
        waiting = []
        vt[...] = kv[1, side, at].T

        def drain():
            b, local, part_total = waiting.pop(0)
            combine(b, p_refs[b % 2][...], local, part_total)

        def finish(b, local, part_total):
            waiting.append((b, local, part_total))
            if len(waiting) > 1:
                drain()

        attend(side, at, lambda b: p_refs[b % 2], finish)
        drain()

    def receive(step, part):
        for way in (1, 0):
            at = 2 * step - 1 + way if step < far else last
            ring(step, part, way).wait_recv()
            if step < far:
                ring(step + 1, part, way).start()
            if step == far:
                to_pair(at, part, way).start()
            elif step > 1:
                to_pair(at, part).start()
            else:
                pl.when(core == 0)(to_pair(at, part).start)

    def met_pair():
        receive(1, 1)

        @pl.when(core == 1)
        def _():
            pl.semaphore_wait(hello, 1)
            for at in (0, 2, 1):
                for part in range(2):
                    to_pair(at, part).start()

    def last_of_pair(part):
        for way in range(2):
            to_pair(last, part, way).wait_recv()

    actions = [
        None,
        lambda: receive(1, 0), met_pair,
        lambda: receive(2, 0), lambda: receive(2, 1),
        lambda: receive(3, 0), lambda: receive(3, 1),
        lambda: receive(4, 0), lambda: last_of_pair(0),
        lambda: receive(4, 1), lambda: last_of_pair(1),
    ]
    turns = []
    for action, zero, one in zip(actions, TURNS[0], TURNS[1], strict=True):
        for k, both in enumerate(zip(zero, one, strict=True)):
            turns.append((*((t % 4, t // 4 % 2, t // 8) for t in both), None if k else action))

    def one(i, _):
        def pick(field):
            found = i * 0
            for k, (zero, one, _) in enumerate(turns):
                value = jnp.where(core == 1, one[field], zero[field])
                found = jnp.where(i == k, value, found)
            return found

        what, side, at = pick(0), pick(1), pick(2)
        for k, (_, _, action) in enumerate(turns):
            if action is not None:
                pl.when(i == k)(action)

        for part in range(2):

            @pl.when(((what == part + 1) | (what == 3)) & (side == 1) & (at != last))
            def _():
                to_pair(at, part).wait_recv()

        pl.when(what == 1)(lambda: weigh_shard(side, at))
        pl.when(what == 2)(lambda: combine_shard(side, at))
        pl.when(what == 3)(lambda: whole_shard(side, at))
        return 0

    pl.semaphore_wait(barrier, 3 - core)

    @pl.when(core == 0)
    def _():
        pl.semaphore_signal(
            hello, inc=1, device_id={"seq": pair}, device_id_type=pl.DeviceIdType.MESH
        )

    for part in range(2):
        for c in own_copies(part):
            c.wait()
        for way in range(2):
            ring(1, part, way).start()

    @pl.when(core == 0)
    def _():
        for part in range(2):
            to_pair(0, part).start()

    for c in q_copies:
        c.wait()
    lax.fori_loop(0, len(turns), one, 0)

    for h in range(GROUP):
        cols = pl.ds(h * span, span)
        out_ref[:, pl.ds(h * DH, DH)] = (
            (acc[:, cols] / total[:, cols]).T.astype(out_ref.dtype)
        )

    for part in range(2):
        for step in range(1, far + 1):
            for way in range(2):
                ring(step, part, way).wait_send()
        for at in range(last):
            to_pair(at, part).wait_send()
        for way in range(2):
            to_pair(last, part, way).wait_send()


def solution(mesh):
    n = mesh.shape["seq"]

    def on_device(queries, new_keys, new_values, cache_keys, cache_values, valid_len, block_of):
        span = queries.shape[0]
        rows = cache_keys.shape[0] + span
        slots = n // 2
        any_spec = pl.BlockSpec(memory_space=pl.ANY)
        smem = pl.BlockSpec(memory_space=pltpu.SMEM)
        return pl.pallas_call(
            functools.partial(kernel, n),
            out_shape=jax.ShapeDtypeStruct(queries.shape, jnp.bfloat16),
            in_specs=[any_spec] * 5 + [smem] * 2,
            out_specs=pl.BlockSpec(memory_space=pltpu.VMEM),
            scratch_shapes=[
                pltpu.VMEM((2, 2, slots, rows, DH), jnp.bfloat16),
                pltpu.VMEM((GROUP * span, 2 * DH), jnp.bfloat16),
                pltpu.VMEM((DH, rows), jnp.bfloat16),
                pltpu.VMEM((rows, DH), jnp.bfloat16),
                pltpu.VMEM((rows, WIDE), jnp.float32),
                pltpu.VMEM((rows, WIDE), jnp.bfloat16),
                pltpu.VMEM((rows, WIDE), jnp.bfloat16),
                pltpu.VMEM((2, slots, GROUP * span // WIDE, rows, WIDE), jnp.bfloat16),
                pltpu.VMEM((2, slots, 1, GROUP * span), jnp.float32),
                pltpu.VMEM((2, slots, 1, GROUP * span), jnp.float32),
                pltpu.VMEM((DH, GROUP * span), jnp.float32),
                pltpu.VMEM((1, GROUP * span), jnp.float32),
                pltpu.VMEM((1, GROUP * span), jnp.float32),
                pltpu.SemaphoreType.REGULAR,
                pltpu.SemaphoreType.DMA((GROUP,)),
                pltpu.SemaphoreType.DMA((2, 2)),
                pltpu.SemaphoreType.DMA((slots // 2, 2, 2)),
                pltpu.SemaphoreType.DMA((slots // 2, 2, 2)),
                pltpu.SemaphoreType.DMA((slots + 1, 2)),
                pltpu.SemaphoreType.DMA((slots + 1, 2)),
            ],
            compiler_params=pltpu.CompilerParams(
                collective_id=0, has_side_effects=True,
                vmem_limit_bytes=60 * 1024 * 1024,
            ),
        )(queries, new_keys, new_values, cache_keys, cache_values, valid_len, block_of)

    rows_spec = P(("groups", "seq"), "head")
    return jax.shard_map(
        on_device,
        mesh=mesh,
        in_specs=(rows_spec,) * 5 + (P("groups"), P("groups")),
        out_specs=rows_spec,
        check_vma=False,
    )
```

```python
import functools
import math

import jax
import jax.numpy as jnp
from jax import lax
from jax.experimental import pallas as pl
from jax.experimental.pallas import tpu as pltpu
from jax.sharding import PartitionSpec as P

DH = 128
GROUP = 8
NEGATIVE = -1e30
FACTOR = DH ** (-0.5) * math.log2(math.e)
WIDE = 256
TALL = 384

TURNS = (
    (
        (3,),
        (7,),
        (17, 9,),
        (18, 10, 23, 15,),
        (33, 25,),
        (34, 26, 39, 31,),
        (49, 41, 53, 45,),
        (50, 42, 54, 46,),
        (57,),
        (61,),
        (58,),
        (62,),
    ),
    (
        (3,),
        (7,),
        (17, 9,),
        (18, 10, 23, 15,),
        (33, 25,),
        (34, 26, 39, 31,),
        (49, 41, 53, 45,),
        (50, 42, 54, 46,),
        (57,),
        (61,),
        (58,),
        (62,),
    ),
)


def kernel(
    n,
    q_hbm, nk_hbm, nv_hbm, ck_hbm, cv_hbm, vl_ref, bo_ref,
    out_ref,
    kv, qs, vt, bias, s_ref, p_even, p_odd, weights, tops, parts, acc, best, total,
    hello, q_sem, own_sem, ring_send, ring_recv, pair_send, pair_recv,
):
    chips = n // 2
    far = chips // 2
    length = ck_hbm.shape[0]
    span = nk_hbm.shape[0]
    rows = length + span
    half = rows // 2
    me = lax.axis_index("seq")
    chip, core = me // 2, me % 2
    right = lax.rem(chip + 1, chips) * 2 + core
    left = lax.rem(chip + chips - 1, chips) * 2 + core
    pair = chip * 2 + 1 - core
    last = 2 * far - 1

    barrier = pltpu.get_barrier_semaphore()

    def greet(peer):
        pl.semaphore_signal(
            barrier, inc=1, device_id={"seq": peer}, device_id_type=pl.DeviceIdType.MESH
        )

    greet(right)
    greet(left)
    pl.when(core == 1)(lambda: greet(pair))

    def own_copies(part):
        cache, fresh = ((ck_hbm, nk_hbm), (cv_hbm, nv_hbm))[part]
        return (
            pltpu.make_async_copy(
                cache, kv.at[part, 0, 0, pl.ds(0, length)], own_sem.at[part, 0]
            ),
            pltpu.make_async_copy(
                fresh, kv.at[part, 0, 0, pl.ds(length, span)], own_sem.at[part, 1]
            ),
        )

    q_copies = [
        pltpu.make_async_copy(
            q_hbm.at[:, pl.ds(h * DH, DH)],
            qs.at[pl.ds(h * span, span), pl.ds(0, DH)],
            q_sem.at[h],
        )
        for h in range(GROUP)
    ]
    for part in range(2):
        for c in own_copies(part):
            c.start()
    for c in q_copies:
        c.start()

    def ring(step, part, way):
        at = 0 if step == 1 else 2 * (step - 1) - 1 + way
        to = 2 * step - 1 + way if step < far else last
        first, count = (0, rows) if step < far else (way * half, half)
        return pltpu.make_async_remote_copy(
            src_ref=kv.at[part, 0, at, pl.ds(first, count)],
            dst_ref=kv.at[part, 0, to, pl.ds(first, count)],
            send_sem=ring_send.at[step - 1, part, way],
            recv_sem=ring_recv.at[step - 1, part, way],
            device_id={"seq": (right, left)[way]},
            device_id_type=pl.DeviceIdType.MESH,
        )

    def to_pair(at, part, way=0):
        first, count = (way * half, half) if at is last else (0, rows)
        return pltpu.make_async_remote_copy(
            src_ref=kv.at[part, 0, at, pl.ds(first, count)],
            dst_ref=kv.at[part, 1, at, pl.ds(first, count)],
            send_sem=pair_send.at[at + way, part],
            recv_sem=pair_recv.at[at + way, part],
            device_id={"seq": pair},
            device_id_type=pl.DeviceIdType.MESH,
        )

    acc[...] = jnp.zeros_like(acc)
    best[...] = jnp.full_like(best, NEGATIVE)
    total[...] = jnp.zeros_like(total)
    place = lax.broadcasted_iota(jnp.int32, (span, DH), 0)
    lane = lax.broadcasted_iota(jnp.int32, (span, DH), 1)
    marks = jnp.where((lane > place) | (lane == 0), 1.0, 0.0).astype(jnp.bfloat16)
    for h in range(GROUP):
        qs[pl.ds(h * span, span), pl.ds(DH, DH)] = marks

    my_block = bo_ref[me]
    blocks = GROUP * span // WIDE
    p_refs = (p_even, p_odd)

    def attend(side, at, weigh_into, finish):
        dist = (at + 1) // 2
        offset = jnp.where(at % 2 == 1, chips - dist, dist)
        shard = lax.rem(chip + offset, chips) * 2 + lax.rem(core + side, 2)
        filled = vl_ref[shard]
        block = bo_ref[shard]
        row = lax.broadcasted_iota(jnp.int32, (length, DH), 0)
        col = lax.broadcasted_iota(jnp.int32, (length, DH), 1)
        bias[pl.ds(0, length), :] = jnp.where(
            (col == 0) & (row >= filled), NEGATIVE, 0.0
        ).astype(jnp.bfloat16)
        hidden_col = jnp.where(block == my_block, place, jnp.where(block < my_block, -1, 0))
        hidden = (lane == hidden_col) & ((place > 0) | (block > my_block))
        bias[pl.ds(length, span), :] = jnp.where(hidden, NEGATIVE, 0.0).astype(jnp.bfloat16)

        local, sums = {}, {}

        def score(b, first):
            s = lax.dot_general(
                jnp.concatenate(
                    [kv[0, side, at, pl.ds(first, TALL), :], bias[pl.ds(first, TALL), :]], axis=1
                ),
                qs[pl.ds(b * WIDE, WIDE), :],
                (((1,), (1,)), ((), ())),
                preferred_element_type=jnp.float32,
            )
            s_ref[pl.ds(first, TALL), :] = s
            high = jnp.max(s.reshape(TALL // 8, 8, WIDE), axis=0)
            local[b] = jnp.maximum(local[b], high) if b in local else high

        def weigh(b, first):
            w = jnp.exp2((s_ref[pl.ds(first, span), :] - local[b]) * FACTOR)
            part = jnp.sum(w.reshape(span // 8, 8, WIDE), axis=0)
            sums[b] = sums[b] + part if b in sums else part
            weigh_into(b)[pl.ds(first, span), :] = w.astype(jnp.bfloat16)

        for b in range(blocks + 1):
            for first in range(0, rows, TALL):
                if b > 0:
                    for inner in range(first, first + TALL, span):
                        weigh(b - 1, inner)
                if b < blocks:
                    score(b, first)
            if b < blocks:
                local[b] = jnp.max(local[b], axis=0, keepdims=True)
            if b > 0:
                finish(b - 1, local[b - 1], jnp.sum(sums[b - 1], axis=0, keepdims=True))

    def combine(b, weighted, local, part_total):
        cols = pl.ds(b * WIDE, WIDE)
        numer = jnp.dot(vt[...], weighted, preferred_element_type=jnp.float32)
        old = best[:, cols]
        newest = jnp.maximum(old, local)
        keep = jnp.exp2((old - newest) * FACTOR)
        fresh = jnp.exp2((local - newest) * FACTOR)
        best[:, cols] = newest
        total[:, cols] = total[:, cols] * keep + part_total * fresh
        acc[:, cols] = acc[:, cols] * keep + numer * fresh

    def weigh_shard(side, at):
        def finish(b, local, part_total):
            cols = pl.ds(b * WIDE, WIDE)
            tops[side, at, :, cols] = local
            parts[side, at, :, cols] = part_total

        attend(side, at, lambda b: weights.at[at + side * 3, b], finish)

    def combine_shard(side, at):
        vt[...] = kv[1, side, at].T
        for b in range(blocks):
            cols = pl.ds(b * WIDE, WIDE)
            combine(b, weights[at + side * 3, b], tops[side, at, :, cols], parts[side, at, :, cols])

    def whole_shard(side, at):
        waiting = []
        vt[...] = kv[1, side, at].T

        def drain():
            b, local, part_total = waiting.pop(0)
            combine(b, p_refs[b % 2][...], local, part_total)

        def finish(b, local, part_total):
            waiting.append((b, local, part_total))
            if len(waiting) > 1:
                drain()

        attend(side, at, lambda b: p_refs[b % 2], finish)
        drain()

    def receive(step, part):
        for way in (1, 0):
            at = 2 * step - 1 + way if step < far else last
            ring(step, part, way).wait_recv()
            if step < far:
                ring(step + 1, part, way).start()
            if step == far:
                to_pair(at, part, way).start()
            else:
                to_pair(at, part).start()

    def meet_pair():
        @pl.when(core == 1)
        def _():
            pl.semaphore_wait(hello, 1)
            for part in range(2):
                to_pair(0, part).start()

    def last_of_pair(part):
        for way in range(2):
            to_pair(last, part, way).wait_recv()

    actions = [
        None, meet_pair,
        lambda: receive(1, 0), lambda: receive(1, 1),
        lambda: receive(2, 0), lambda: receive(2, 1),
        lambda: receive(3, 0), lambda: receive(3, 1),
        lambda: receive(4, 0), lambda: last_of_pair(0),
        lambda: receive(4, 1), lambda: last_of_pair(1),
    ]
    turns = []
    for action, zero, one in zip(actions, TURNS[0], TURNS[1], strict=True):
        for k, both in enumerate(zip(zero, one, strict=True)):
            turns.append((*((t % 4, t // 4 % 2, t // 8) for t in both), None if k else action))

    def one(i, _):
        def pick(field):
            found = i * 0
            for k, (zero, one, _) in enumerate(turns):
                value = jnp.where(core == 1, one[field], zero[field])
                found = jnp.where(i == k, value, found)
            return found

        what, side, at = pick(0), pick(1), pick(2)
        for k, (_, _, action) in enumerate(turns):
            if action is not None:
                pl.when(i == k)(action)

        for part in range(2):

            @pl.when(((what == part + 1) | (what == 3)) & (side == 1) & (at != last))
            def _():
                to_pair(at, part).wait_recv()

        pl.when(what == 1)(lambda: weigh_shard(side, at))
        pl.when(what == 2)(lambda: combine_shard(side, at))
        pl.when(what == 3)(lambda: whole_shard(side, at))
        return 0

    pl.semaphore_wait(barrier, 3 - core)

    @pl.when(core == 0)
    def _():
        pl.semaphore_signal(
            hello, inc=1, device_id={"seq": pair}, device_id_type=pl.DeviceIdType.MESH
        )

    for part in range(2):
        for c in own_copies(part):
            c.wait()
        for way in range(2):
            ring(1, part, way).start()

    @pl.when(core == 0)
    def _():
        for part in range(2):
            to_pair(0, part).start()

    for c in q_copies:
        c.wait()
    lax.fori_loop(0, len(turns), one, 0)

    for h in range(GROUP):
        cols = pl.ds(h * span, span)
        out_ref[:, pl.ds(h * DH, DH)] = (
            (acc[:, cols] / total[:, cols]).T.astype(out_ref.dtype)
        )

    for part in range(2):
        for step in range(1, far + 1):
            for way in range(2):
                ring(step, part, way).wait_send()
        for at in range(last):
            to_pair(at, part).wait_send()
        for way in range(2):
            to_pair(last, part, way).wait_send()


def solution(mesh):
    n = mesh.shape["seq"]

    def on_device(queries, new_keys, new_values, cache_keys, cache_values, valid_len, block_of):
        span = queries.shape[0]
        rows = cache_keys.shape[0] + span
        slots = n // 2
        any_spec = pl.BlockSpec(memory_space=pltpu.HBM)
        smem = pl.BlockSpec(memory_space=pltpu.SMEM)
        return pl.pallas_call(
            functools.partial(kernel, n),
            out_shape=pltpu.VMEM(queries.shape, jnp.bfloat16),
            in_specs=[any_spec] * 5 + [smem] * 2,
            out_specs=pl.BlockSpec(memory_space=pltpu.VMEM),
            scratch_shapes=[
                pltpu.VMEM((2, 2, slots, rows, DH), jnp.bfloat16),
                pltpu.VMEM((GROUP * span, 2 * DH), jnp.bfloat16),
                pltpu.VMEM((DH, rows), jnp.bfloat16),
                pltpu.VMEM((rows, DH), jnp.bfloat16),
                pltpu.VMEM((rows, WIDE), jnp.float32),
                pltpu.VMEM((rows, WIDE), jnp.bfloat16),
                pltpu.VMEM((rows, WIDE), jnp.bfloat16),
                pltpu.VMEM((slots + 3, GROUP * span // WIDE, rows, WIDE), jnp.bfloat16),
                pltpu.VMEM((2, slots, 1, GROUP * span), jnp.float32),
                pltpu.VMEM((2, slots, 1, GROUP * span), jnp.float32),
                pltpu.VMEM((DH, GROUP * span), jnp.float32),
                pltpu.VMEM((1, GROUP * span), jnp.float32),
                pltpu.VMEM((1, GROUP * span), jnp.float32),
                pltpu.SemaphoreType.REGULAR,
                pltpu.SemaphoreType.DMA((GROUP,)),
                pltpu.SemaphoreType.DMA((2, 2)),
                pltpu.SemaphoreType.DMA((slots // 2, 2, 2)),
                pltpu.SemaphoreType.DMA((slots // 2, 2, 2)),
                pltpu.SemaphoreType.DMA((slots + 1, 2)),
                pltpu.SemaphoreType.DMA((slots + 1, 2)),
            ],
            compiler_params=pltpu.CompilerParams(
                collective_id=0, has_side_effects=True,
                vmem_limit_bytes=60 * 1024 * 1024,
            ),
        )(queries, new_keys, new_values, cache_keys, cache_values, valid_len, block_of)

    rows_spec = P(("groups", "seq"), "head")
    return jax.shard_map(
        on_device,
        mesh=mesh,
        in_specs=(rows_spec,) * 5 + (P("groups"), P("groups")),
        out_specs=rows_spec,
        check_vma=False,
    )
```

```python
import functools
import math

import jax
import jax.numpy as jnp
from jax import lax
from jax.experimental import pallas as pl
from jax.experimental.pallas import tpu as pltpu
from jax.sharding import PartitionSpec as P

DH = 128
GROUP = 8
NEGATIVE = -1e30
FACTOR = DH ** (-0.5) * math.log2(math.e)
WIDE = 256
TALL = 384

TURNS = (
    (
        (3,),
        (17, 9,),
        (7,),
        (18, 10, 23, 15,),
        (33, 25,),
        (34, 26, 39, 31,),
        (49, 41, 53, 45,),
        (50, 42, 54, 46,),
        (57,),
        (61,),
        (58,),
        (62,),
    ),
    (
        (3,),
        (17, 9,),
        (7,),
        (18, 10, 23, 15,),
        (33, 25,),
        (34, 26, 39, 31,),
        (49, 41, 53, 45,),
        (50, 42, 54, 46,),
        (57,),
        (61,),
        (58,),
        (62,),
    ),
)


def kernel(
    n,
    q_hbm, nk_hbm, nv_hbm, ck_hbm, cv_hbm, vl_ref, bo_ref,
    out_ref,
    kv, qs, vt, bias, s_ref, p_even, p_odd, weights, tops, parts, acc, best, total,
    hello, q_sem, own_sem, ring_send, ring_recv, pair_send, pair_recv,
):
    chips = n // 2
    far = chips // 2
    length = ck_hbm.shape[0]
    span = nk_hbm.shape[0]
    rows = length + span
    half = rows // 2
    me = lax.axis_index("seq")
    chip, core = me // 2, me % 2
    right = lax.rem(chip + 1, chips) * 2 + core
    left = lax.rem(chip + chips - 1, chips) * 2 + core
    pair = chip * 2 + 1 - core
    last = 2 * far - 1

    barrier = pltpu.get_barrier_semaphore()

    def greet(peer):
        pl.semaphore_signal(
            barrier, inc=1, device_id={"seq": peer}, device_id_type=pl.DeviceIdType.MESH
        )

    greet(right)
    greet(left)
    pl.when(core == 1)(lambda: greet(pair))

    def own_copies(part):
        cache, fresh = ((ck_hbm, nk_hbm), (cv_hbm, nv_hbm))[part]
        return (
            pltpu.make_async_copy(
                cache, kv.at[part, 0, 0, pl.ds(0, length)], own_sem.at[part, 0]
            ),
            pltpu.make_async_copy(
                fresh, kv.at[part, 0, 0, pl.ds(length, span)], own_sem.at[part, 1]
            ),
        )

    q_copies = [
        pltpu.make_async_copy(
            q_hbm.at[:, pl.ds(h * DH, DH)],
            qs.at[pl.ds(h * span, span), pl.ds(0, DH)],
            q_sem.at[h],
        )
        for h in range(GROUP)
    ]
    for part in range(2):
        for c in own_copies(part):
            c.start()
    for c in q_copies:
        c.start()

    def ring(step, part, way):
        at = 0 if step == 1 else 2 * (step - 1) - 1 + way
        to = 2 * step - 1 + way if step < far else last
        first, count = (0, rows) if step < far else (way * half, half)
        return pltpu.make_async_remote_copy(
            src_ref=kv.at[part, 0, at, pl.ds(first, count)],
            dst_ref=kv.at[part, 0, to, pl.ds(first, count)],
            send_sem=ring_send.at[step - 1, part, way],
            recv_sem=ring_recv.at[step - 1, part, way],
            device_id={"seq": (right, left)[way]},
            device_id_type=pl.DeviceIdType.MESH,
        )

    def to_pair(at, part, way=0):
        first, count = (way * half, half) if at is last else (0, rows)
        return pltpu.make_async_remote_copy(
            src_ref=kv.at[part, 0, at, pl.ds(first, count)],
            dst_ref=kv.at[part, 1, at, pl.ds(first, count)],
            send_sem=pair_send.at[at + way, part],
            recv_sem=pair_recv.at[at + way, part],
            device_id={"seq": pair},
            device_id_type=pl.DeviceIdType.MESH,
        )

    acc[...] = jnp.zeros_like(acc)
    best[...] = jnp.full_like(best, NEGATIVE)
    total[...] = jnp.zeros_like(total)
    place = lax.broadcasted_iota(jnp.int32, (span, DH), 0)
    lane = lax.broadcasted_iota(jnp.int32, (span, DH), 1)
    marks = jnp.where((lane > place) | (lane == 0), 1.0, 0.0).astype(jnp.bfloat16)
    for h in range(GROUP):
        qs[pl.ds(h * span, span), pl.ds(DH, DH)] = marks

    my_block = bo_ref[me]
    blocks = GROUP * span // WIDE
    p_refs = (p_even, p_odd)

    def attend(side, at, weigh_into, finish):
        dist = (at + 1) // 2
        offset = jnp.where(at % 2 == 1, chips - dist, dist)
        shard = lax.rem(chip + offset, chips) * 2 + lax.rem(core + side, 2)
        filled = vl_ref[shard]
        block = bo_ref[shard]
        row = lax.broadcasted_iota(jnp.int32, (length, DH), 0)
        col = lax.broadcasted_iota(jnp.int32, (length, DH), 1)
        bias[pl.ds(0, length), :] = jnp.where(
            (col == 0) & (row >= filled), NEGATIVE, 0.0
        ).astype(jnp.bfloat16)
        hidden_col = jnp.where(block == my_block, place, jnp.where(block < my_block, -1, 0))
        hidden = (lane == hidden_col) & ((place > 0) | (block > my_block))
        bias[pl.ds(length, span), :] = jnp.where(hidden, NEGATIVE, 0.0).astype(jnp.bfloat16)

        local, sums = {}, {}

        def score(b, first):
            s = lax.dot_general(
                jnp.concatenate(
                    [kv[0, side, at, pl.ds(first, TALL), :], bias[pl.ds(first, TALL), :]], axis=1
                ),
                qs[pl.ds(b * WIDE, WIDE), :],
                (((1,), (1,)), ((), ())),
                preferred_element_type=jnp.float32,
            )
            s_ref[pl.ds(first, TALL), :] = s
            high = jnp.max(s.reshape(TALL // 8, 8, WIDE), axis=0)
            local[b] = jnp.maximum(local[b], high) if b in local else high

        def weigh(b, first):
            w = jnp.exp2((s_ref[pl.ds(first, span), :] - local[b]) * FACTOR)
            part = jnp.sum(w.reshape(span // 8, 8, WIDE), axis=0)
            sums[b] = sums[b] + part if b in sums else part
            weigh_into(b)[pl.ds(first, span), :] = w.astype(jnp.bfloat16)

        for b in range(blocks + 1):
            for first in range(0, rows, TALL):
                if b > 0:
                    for inner in range(first, first + TALL, span):
                        weigh(b - 1, inner)
                if b < blocks:
                    score(b, first)
            if b < blocks:
                local[b] = jnp.max(local[b], axis=0, keepdims=True)
            if b > 0:
                finish(b - 1, local[b - 1], jnp.sum(sums[b - 1], axis=0, keepdims=True))

    def combine(b, weighted, local, part_total):
        cols = pl.ds(b * WIDE, WIDE)
        numer = jnp.dot(vt[...], weighted, preferred_element_type=jnp.float32)
        old = best[:, cols]
        newest = jnp.maximum(old, local)
        keep = jnp.exp2((old - newest) * FACTOR)
        fresh = jnp.exp2((local - newest) * FACTOR)
        best[:, cols] = newest
        total[:, cols] = total[:, cols] * keep + part_total * fresh
        acc[:, cols] = acc[:, cols] * keep + numer * fresh

    def weigh_shard(side, at):
        def finish(b, local, part_total):
            cols = pl.ds(b * WIDE, WIDE)
            tops[side, at, :, cols] = local
            parts[side, at, :, cols] = part_total

        attend(side, at, lambda b: weights.at[at + side * 3, b], finish)

    def combine_shard(side, at):
        vt[...] = kv[1, side, at].T
        for b in range(blocks):
            cols = pl.ds(b * WIDE, WIDE)
            combine(b, weights[at + side * 3, b], tops[side, at, :, cols], parts[side, at, :, cols])

    def whole_shard(side, at):
        waiting = []
        vt[...] = kv[1, side, at].T

        def drain():
            b, local, part_total = waiting.pop(0)
            combine(b, p_refs[b % 2][...], local, part_total)

        def finish(b, local, part_total):
            waiting.append((b, local, part_total))
            if len(waiting) > 1:
                drain()

        attend(side, at, lambda b: p_refs[b % 2], finish)
        drain()

    def receive(step, part):
        for way in (1, 0):
            at = 2 * step - 1 + way if step < far else last
            ring(step, part, way).wait_recv()
            if step < far:
                ring(step + 1, part, way).start()
            if step == far:
                to_pair(at, part, way).start()
            elif step == 1 and part == 0:
                pl.when(core == 0)(to_pair(at, part).start)
            else:
                to_pair(at, part).start()

    def meet_pair():
        @pl.when(core == 1)
        def _():
            pl.semaphore_wait(hello, 1)
            for at, part in ((0, 0), (0, 1), (2, 0), (1, 0)):
                to_pair(at, part).start()

    def last_of_pair(part):
        for way in range(2):
            to_pair(last, part, way).wait_recv()

    actions = [
        None, lambda: receive(1, 0),
        meet_pair, lambda: receive(1, 1),
        lambda: receive(2, 0), lambda: receive(2, 1),
        lambda: receive(3, 0), lambda: receive(3, 1),
        lambda: receive(4, 0), lambda: last_of_pair(0),
        lambda: receive(4, 1), lambda: last_of_pair(1),
    ]
    turns = []
    for action, zero, one in zip(actions, TURNS[0], TURNS[1], strict=True):
        for k, both in enumerate(zip(zero, one, strict=True)):
            turns.append((*((t % 4, t // 4 % 2, t // 8) for t in both), None if k else action))

    def one(i, _):
        def pick(field):
            found = i * 0
            for k, (zero, one, _) in enumerate(turns):
                value = jnp.where(core == 1, one[field], zero[field])
                found = jnp.where(i == k, value, found)
            return found

        what, side, at = pick(0), pick(1), pick(2)
        for k, (_, _, action) in enumerate(turns):
            if action is not None:
                pl.when(i == k)(action)

        for part in range(2):

            @pl.when(((what == part + 1) | (what == 3)) & (side == 1) & (at != last))
            def _():
                to_pair(at, part).wait_recv()

        pl.when(what == 1)(lambda: weigh_shard(side, at))
        pl.when(what == 2)(lambda: combine_shard(side, at))
        pl.when(what == 3)(lambda: whole_shard(side, at))
        return 0

    pl.semaphore_wait(barrier, 3 - core)

    @pl.when(core == 0)
    def _():
        pl.semaphore_signal(
            hello, inc=1, device_id={"seq": pair}, device_id_type=pl.DeviceIdType.MESH
        )

    for part in range(2):
        for c in own_copies(part):
            c.wait()
        for way in range(2):
            ring(1, part, way).start()

    @pl.when(core == 0)
    def _():
        for part in range(2):
            to_pair(0, part).start()

    for c in q_copies:
        c.wait()
    lax.fori_loop(0, len(turns), one, 0)

    for h in range(GROUP):
        cols = pl.ds(h * span, span)
        out_ref[:, pl.ds(h * DH, DH)] = (
            (acc[:, cols] / total[:, cols]).T.astype(out_ref.dtype)
        )

    for part in range(2):
        for step in range(1, far + 1):
            for way in range(2):
                ring(step, part, way).wait_send()
        for at in range(last):
            to_pair(at, part).wait_send()
        for way in range(2):
            to_pair(last, part, way).wait_send()


def solution(mesh):
    n = mesh.shape["seq"]

    def on_device(queries, new_keys, new_values, cache_keys, cache_values, valid_len, block_of):
        span = queries.shape[0]
        rows = cache_keys.shape[0] + span
        slots = n // 2
        any_spec = pl.BlockSpec(memory_space=pltpu.HBM)
        smem = pl.BlockSpec(memory_space=pltpu.SMEM)
        return pl.pallas_call(
            functools.partial(kernel, n),
            out_shape=pltpu.VMEM(queries.shape, jnp.bfloat16),
            in_specs=[any_spec] * 5 + [smem] * 2,
            out_specs=pl.BlockSpec(memory_space=pltpu.VMEM),
            scratch_shapes=[
                pltpu.VMEM((2, 2, slots, rows, DH), jnp.bfloat16),
                pltpu.VMEM((GROUP * span, 2 * DH), jnp.bfloat16),
                pltpu.VMEM((DH, rows), jnp.bfloat16),
                pltpu.VMEM((rows, DH), jnp.bfloat16),
                pltpu.VMEM((rows, WIDE), jnp.float32),
                pltpu.VMEM((rows, WIDE), jnp.bfloat16),
                pltpu.VMEM((rows, WIDE), jnp.bfloat16),
                pltpu.VMEM((slots + 3, GROUP * span // WIDE, rows, WIDE), jnp.bfloat16),
                pltpu.VMEM((2, slots, 1, GROUP * span), jnp.float32),
                pltpu.VMEM((2, slots, 1, GROUP * span), jnp.float32),
                pltpu.VMEM((DH, GROUP * span), jnp.float32),
                pltpu.VMEM((1, GROUP * span), jnp.float32),
                pltpu.VMEM((1, GROUP * span), jnp.float32),
                pltpu.SemaphoreType.REGULAR,
                pltpu.SemaphoreType.DMA((GROUP,)),
                pltpu.SemaphoreType.DMA((2, 2)),
                pltpu.SemaphoreType.DMA((slots // 2, 2, 2)),
                pltpu.SemaphoreType.DMA((slots // 2, 2, 2)),
                pltpu.SemaphoreType.DMA((slots + 1, 2)),
                pltpu.SemaphoreType.DMA((slots + 1, 2)),
            ],
            compiler_params=pltpu.CompilerParams(
                collective_id=0, has_side_effects=True,
                vmem_limit_bytes=60 * 1024 * 1024,
            ),
        )(queries, new_keys, new_values, cache_keys, cache_values, valid_len, block_of)

    rows_spec = P(("groups", "seq"), "head")
    return jax.shard_map(
        on_device,
        mesh=mesh,
        in_specs=(rows_spec,) * 5 + (P("groups"), P("groups")),
        out_specs=rows_spec,
        check_vma=False,
    )
```

```python
import functools
import math

import jax
import jax.numpy as jnp
from jax import lax
from jax.experimental import pallas as pl
from jax.experimental.pallas import tpu as pltpu
from jax.sharding import PartitionSpec as P

DH = 128
GROUP = 8
NEGATIVE = -1e30
FACTOR = DH ** (-0.5) * math.log2(math.e)
WIDE = 256
TALL = 384

TURNS = (
    (
        (3,),
        (17, 9,),
        (7,),
        (18, 10, 23,),
        (33, 25, 15,),
        (34, 26, 39, 31,),
        (49, 41, 53, 45,),
        (50, 42, 54, 46,),
        (57,),
        (61,),
        (58,),
        (62,),
    ),
    (
        (3,),
        (17, 9,),
        (7,),
        (18, 10, 23,),
        (33, 25, 15,),
        (34, 26, 39, 31,),
        (49, 41, 53, 45,),
        (50, 42, 54, 46,),
        (57,),
        (61,),
        (58,),
        (62,),
    ),
)


def kernel(
    n,
    q_hbm, nk_hbm, nv_hbm, ck_hbm, cv_hbm, vl_ref, bo_ref,
    out_ref,
    kv, qs, vt, bias, s_ref, p_even, p_odd, weights, tops, parts, acc, best, total,
    hello, q_sem, own_sem, ring_send, ring_recv, pair_send, pair_recv,
):
    chips = n // 2
    far = chips // 2
    length = ck_hbm.shape[0]
    span = nk_hbm.shape[0]
    rows = length + span
    half = rows // 2
    me = lax.axis_index("seq")
    chip, core = me // 2, me % 2
    right = lax.rem(chip + 1, chips) * 2 + core
    left = lax.rem(chip + chips - 1, chips) * 2 + core
    pair = chip * 2 + 1 - core
    last = 2 * far - 1

    barrier = pltpu.get_barrier_semaphore()

    def greet(peer):
        pl.semaphore_signal(
            barrier, inc=1, device_id={"seq": peer}, device_id_type=pl.DeviceIdType.MESH
        )

    greet(right)
    greet(left)
    pl.when(core == 1)(lambda: greet(pair))

    def own_copies(part):
        cache, fresh = ((ck_hbm, nk_hbm), (cv_hbm, nv_hbm))[part]
        return (
            pltpu.make_async_copy(
                cache, kv.at[part, 0, 0, pl.ds(0, length)], own_sem.at[part, 0]
            ),
            pltpu.make_async_copy(
                fresh, kv.at[part, 0, 0, pl.ds(length, span)], own_sem.at[part, 1]
            ),
        )

    q_copies = [
        pltpu.make_async_copy(
            q_hbm.at[:, pl.ds(h * DH, DH)],
            qs.at[pl.ds(h * span, span), pl.ds(0, DH)],
            q_sem.at[h],
        )
        for h in range(GROUP)
    ]
    for part in range(2):
        for c in own_copies(part):
            c.start()
    for c in q_copies:
        c.start()

    def ring(step, part, way):
        at = 0 if step == 1 else 2 * (step - 1) - 1 + way
        to = 2 * step - 1 + way if step < far else last
        first, count = (0, rows) if step < far else (way * half, half)
        return pltpu.make_async_remote_copy(
            src_ref=kv.at[part, 0, at, pl.ds(first, count)],
            dst_ref=kv.at[part, 0, to, pl.ds(first, count)],
            send_sem=ring_send.at[step - 1, part, way],
            recv_sem=ring_recv.at[step - 1, part, way],
            device_id={"seq": (right, left)[way]},
            device_id_type=pl.DeviceIdType.MESH,
        )

    def to_pair(at, part, way=0):
        first, count = (way * half, half) if at is last else (0, rows)
        return pltpu.make_async_remote_copy(
            src_ref=kv.at[part, 0, at, pl.ds(first, count)],
            dst_ref=kv.at[part, 1, at, pl.ds(first, count)],
            send_sem=pair_send.at[at + way, part],
            recv_sem=pair_recv.at[at + way, part],
            device_id={"seq": pair},
            device_id_type=pl.DeviceIdType.MESH,
        )

    acc[...] = jnp.zeros_like(acc)
    best[...] = jnp.full_like(best, NEGATIVE)
    total[...] = jnp.zeros_like(total)
    place = lax.broadcasted_iota(jnp.int32, (span, DH), 0)
    lane = lax.broadcasted_iota(jnp.int32, (span, DH), 1)
    marks = jnp.where((lane > place) | (lane == 0), 1.0, 0.0).astype(jnp.bfloat16)
    for h in range(GROUP):
        qs[pl.ds(h * span, span), pl.ds(DH, DH)] = marks

    my_block = bo_ref[me]
    blocks = GROUP * span // WIDE
    p_refs = (p_even, p_odd)

    def attend(side, at, weigh_into, finish):
        dist = (at + 1) // 2
        offset = jnp.where(at % 2 == 1, chips - dist, dist)
        shard = lax.rem(chip + offset, chips) * 2 + lax.rem(core + side, 2)
        filled = vl_ref[shard]
        block = bo_ref[shard]
        row = lax.broadcasted_iota(jnp.int32, (length, DH), 0)
        col = lax.broadcasted_iota(jnp.int32, (length, DH), 1)
        bias[pl.ds(0, length), :] = jnp.where(
            (col == 0) & (row >= filled), NEGATIVE, 0.0
        ).astype(jnp.bfloat16)
        hidden_col = jnp.where(block == my_block, place, jnp.where(block < my_block, -1, 0))
        hidden = (lane == hidden_col) & ((place > 0) | (block > my_block))
        bias[pl.ds(length, span), :] = jnp.where(hidden, NEGATIVE, 0.0).astype(jnp.bfloat16)

        local, sums = {}, {}

        def score(b, first):
            s = lax.dot_general(
                jnp.concatenate(
                    [kv[0, side, at, pl.ds(first, TALL), :], bias[pl.ds(first, TALL), :]], axis=1
                ),
                qs[pl.ds(b * WIDE, WIDE), :],
                (((1,), (1,)), ((), ())),
                preferred_element_type=jnp.float32,
            )
            s_ref[pl.ds(first, TALL), :] = s
            high = jnp.max(s.reshape(TALL // 8, 8, WIDE), axis=0)
            local[b] = jnp.maximum(local[b], high) if b in local else high

        def weigh(b, first):
            w = jnp.exp2((s_ref[pl.ds(first, span), :] - local[b]) * FACTOR)
            part = jnp.sum(w.reshape(span // 8, 8, WIDE), axis=0)
            sums[b] = sums[b] + part if b in sums else part
            weigh_into(b)[pl.ds(first, span), :] = w.astype(jnp.bfloat16)

        for b in range(blocks + 1):
            for first in range(0, rows, TALL):
                if b > 0:
                    for inner in range(first, first + TALL, span):
                        weigh(b - 1, inner)
                if b < blocks:
                    score(b, first)
            if b < blocks:
                local[b] = jnp.max(local[b], axis=0, keepdims=True)
            if b > 0:
                finish(b - 1, local[b - 1], jnp.sum(sums[b - 1], axis=0, keepdims=True))

    def combine(b, weighted, local, part_total):
        cols = pl.ds(b * WIDE, WIDE)
        numer = jnp.dot(vt[...], weighted, preferred_element_type=jnp.float32)
        old = best[:, cols]
        newest = jnp.maximum(old, local)
        keep = jnp.exp2((old - newest) * FACTOR)
        fresh = jnp.exp2((local - newest) * FACTOR)
        best[:, cols] = newest
        total[:, cols] = total[:, cols] * keep + part_total * fresh
        acc[:, cols] = acc[:, cols] * keep + numer * fresh

    def weigh_shard(side, at):
        def finish(b, local, part_total):
            cols = pl.ds(b * WIDE, WIDE)
            tops[side, at, :, cols] = local
            parts[side, at, :, cols] = part_total

        attend(side, at, lambda b: weights.at[at + side * 3, b], finish)

    def combine_shard(side, at):
        vt[...] = kv[1, side, at].T
        for b in range(blocks):
            cols = pl.ds(b * WIDE, WIDE)
            combine(b, weights[at + side * 3, b], tops[side, at, :, cols], parts[side, at, :, cols])

    def whole_shard(side, at):
        waiting = []
        vt[...] = kv[1, side, at].T

        def drain():
            b, local, part_total = waiting.pop(0)
            combine(b, p_refs[b % 2][...], local, part_total)

        def finish(b, local, part_total):
            waiting.append((b, local, part_total))
            if len(waiting) > 1:
                drain()

        attend(side, at, lambda b: p_refs[b % 2], finish)
        drain()

    def receive(step, part):
        for way in (1, 0):
            at = 2 * step - 1 + way if step < far else last
            ring(step, part, way).wait_recv()
            if step < far:
                ring(step + 1, part, way).start()
            if step == far:
                to_pair(at, part, way).start()
            elif step == 1 and part == 0:
                pl.when(core == 0)(to_pair(at, part).start)
            else:
                to_pair(at, part).start()

    def meet_pair():
        @pl.when(core == 1)
        def _():
            pl.semaphore_wait(hello, 1)
            for at, part in ((0, 0), (0, 1), (2, 0), (1, 0)):
                to_pair(at, part).start()

    def last_of_pair(part):
        for way in range(2):
            to_pair(last, part, way).wait_recv()

    actions = [
        None, lambda: receive(1, 0),
        meet_pair, lambda: receive(1, 1),
        lambda: receive(2, 0), lambda: receive(2, 1),
        lambda: receive(3, 0), lambda: receive(3, 1),
        lambda: receive(4, 0), lambda: last_of_pair(0),
        lambda: receive(4, 1), lambda: last_of_pair(1),
    ]
    turns = []
    for action, zero, one in zip(actions, TURNS[0], TURNS[1], strict=True):
        for k, both in enumerate(zip(zero, one, strict=True)):
            turns.append((*((t % 4, t // 4 % 2, t // 8) for t in both), None if k else action))

    def one(i, _):
        def pick(field):
            found = i * 0
            for k, (zero, one, _) in enumerate(turns):
                value = jnp.where(core == 1, one[field], zero[field])
                found = jnp.where(i == k, value, found)
            return found

        what, side, at = pick(0), pick(1), pick(2)
        for k, (_, _, action) in enumerate(turns):
            if action is not None:
                pl.when(i == k)(action)

        for part in range(2):

            @pl.when(((what == part + 1) | (what == 3)) & (side == 1) & (at != last))
            def _():
                to_pair(at, part).wait_recv()

        pl.when(what == 1)(lambda: weigh_shard(side, at))
        pl.when(what == 2)(lambda: combine_shard(side, at))
        pl.when(what == 3)(lambda: whole_shard(side, at))
        return 0

    pl.semaphore_wait(barrier, 3 - core)

    @pl.when(core == 0)
    def _():
        pl.semaphore_signal(
            hello, inc=1, device_id={"seq": pair}, device_id_type=pl.DeviceIdType.MESH
        )

    for part in range(2):
        for c in own_copies(part):
            c.wait()
        for way in range(2):
            ring(1, part, way).start()

    @pl.when(core == 0)
    def _():
        for part in range(2):
            to_pair(0, part).start()

    for c in q_copies:
        c.wait()
    lax.fori_loop(0, len(turns), one, 0)

    for h in range(GROUP):
        cols = pl.ds(h * span, span)
        out_ref[:, pl.ds(h * DH, DH)] = (
            (acc[:, cols] / total[:, cols]).T.astype(out_ref.dtype)
        )

    for part in range(2):
        for step in range(1, far + 1):
            for way in range(2):
                ring(step, part, way).wait_send()
        for at in range(last):
            to_pair(at, part).wait_send()
        for way in range(2):
            to_pair(last, part, way).wait_send()


def solution(mesh):
    n = mesh.shape["seq"]

    def on_device(queries, new_keys, new_values, cache_keys, cache_values, valid_len, block_of):
        span = queries.shape[0]
        rows = cache_keys.shape[0] + span
        slots = n // 2
        any_spec = pl.BlockSpec(memory_space=pltpu.HBM)
        smem = pl.BlockSpec(memory_space=pltpu.SMEM)
        return pl.pallas_call(
            functools.partial(kernel, n),
            out_shape=pltpu.VMEM(queries.shape, jnp.bfloat16),
            in_specs=[any_spec] * 5 + [smem] * 2,
            out_specs=pl.BlockSpec(memory_space=pltpu.VMEM),
            scratch_shapes=[
                pltpu.VMEM((2, 2, slots, rows, DH), jnp.bfloat16),
                pltpu.VMEM((GROUP * span, 2 * DH), jnp.bfloat16),
                pltpu.VMEM((DH, rows), jnp.bfloat16),
                pltpu.VMEM((rows, DH), jnp.bfloat16),
                pltpu.VMEM((rows, WIDE), jnp.float32),
                pltpu.VMEM((rows, WIDE), jnp.bfloat16),
                pltpu.VMEM((rows, WIDE), jnp.bfloat16),
                pltpu.VMEM((slots + 3, GROUP * span // WIDE, rows, WIDE), jnp.bfloat16),
                pltpu.VMEM((2, slots, 1, GROUP * span), jnp.float32),
                pltpu.VMEM((2, slots, 1, GROUP * span), jnp.float32),
                pltpu.VMEM((DH, GROUP * span), jnp.float32),
                pltpu.VMEM((1, GROUP * span), jnp.float32),
                pltpu.VMEM((1, GROUP * span), jnp.float32),
                pltpu.SemaphoreType.REGULAR,
                pltpu.SemaphoreType.DMA((GROUP,)),
                pltpu.SemaphoreType.DMA((2, 2)),
                pltpu.SemaphoreType.DMA((slots // 2, 2, 2)),
                pltpu.SemaphoreType.DMA((slots // 2, 2, 2)),
                pltpu.SemaphoreType.DMA((slots + 1, 2)),
                pltpu.SemaphoreType.DMA((slots + 1, 2)),
            ],
            compiler_params=pltpu.CompilerParams(
                collective_id=0, has_side_effects=True,
                vmem_limit_bytes=60 * 1024 * 1024,
            ),
        )(queries, new_keys, new_values, cache_keys, cache_values, valid_len, block_of)

    rows_spec = P(("groups", "seq"), "head")
    return jax.shard_map(
        on_device,
        mesh=mesh,
        in_specs=(rows_spec,) * 5 + (P("groups"), P("groups")),
        out_specs=rows_spec,
        check_vma=False,
    )
```
